32 devices in a mesh: section: 4 (over y, x), dp: 8 (over z, core).
Axes of the slice: x: 2, y: 2, z: 4, core: 2. Of those that a mesh axis runs over, the one named last changes fastest.
Arguments:
- owner_table: int32 [4, 4], P('section'), may hold values from 0 to 3, each once within a row
- hidden_acts: bfloat16 [4, 1024, 2048], P('section', 'dp'), may hold values from -6 to 6
- sent_grad: bfloat16 [4, 1024, 512], P('section', 'dp'), may hold values from -0.25 to 0.25
Outputs:
- update: bfloat16 [4, 4, 512, 512], P('section')
The draws below stay inside these ranges and needn't reach their ends.
Inputs may be any that keep to these rules, and one draw needn't show every extreme that they name: `owner_table`: each section's row is a permutation of 0 to 3.
All inputs are finite; a program needn't handle non-finite values.
Results may differ from the reference program's by a relative error of at most 0.0098.
Values may be sent and summed in bfloat16 or wider, within the bound.
No kernel may reach another device: no remote copies, remote signals or barrier semaphores. Data moves between devices by JAX's collectives and lax.ppermute only.
A program may use at most 64 MiB of HBM per device.

```python
import jax
import jax.numpy as jnp
from jax import lax

BLK = 512
NB = 4
ITERS = 2
SECTIONS = 4
TOKENS = 1024


def with_spikes(values, key, source, target, blocks, factor):
    def block_of(axis_at):
        return (jnp.arange(values.shape[axis_at]) // (values.shape[axis_at] // blocks)).reshape((-1,) + (1,) * (values.ndim - 1 - axis_at))

    near = jax.random.permutation(key, blocks)[block_of(target)]
    other_side = (block_of(target) + blocks // 2) % blocks
    return jnp.where((block_of(source) == near) | (block_of(source) == other_side), factor * values, values)


def block_scale(key, extent, split, least, largest):
    gain, own = 1.0, jax.random.fold_in(key, 6)
    for axis_at, blocks in split:
        steps = jnp.exp(jax.random.uniform(jax.random.fold_in(own, axis_at), (blocks,), jnp.float32, least / len(split), largest / len(split)))
        gain = gain * jnp.repeat(steps, extent[axis_at] // blocks).reshape([-1 if axis == axis_at else 1 for axis in range(len(extent))])
    return gain


def gaussian(rng, dims, width, reach, split=(), kind=jnp.bfloat16):
    factor_of = block_scale(rng, dims, split, -0.22, 0.18) if split else 1.0
    array = jax.random.normal(rng, dims, jnp.float32) * width * factor_of
    return jnp.minimum(jnp.maximum(array, -reach), reach).astype(kind)


def heavy_noise(stream_key, extent, scale, reach, cuts, heavy, kind=jnp.bfloat16):
    values = scale * jax.random.normal(stream_key, extent, jnp.float32)
    if cuts:
        values = values * block_scale(stream_key, extent, cuts, -0.22, 0.18)
    return jnp.clip(with_spikes(values, jax.random.fold_in(stream_key, 3), *heavy), -reach, reach).astype(kind)


def setup_inputs(seed: int = 0) -> dict:
    seeds = jax.random.split(jax.random.key(seed), 4)
    owner_table = jax.vmap(lambda own: jax.random.permutation(own, NB))(jax.random.split(seeds[0], SECTIONS)).reshape((SECTIONS, NB)).astype(jnp.int32)
    hidden_acts = gaussian(seeds[1], (SECTIONS, TOKENS, NB * BLK), 1.0, 6.0, ((0, 4), (1, 8)))
    sent_grad = heavy_noise(seeds[2], (SECTIONS, TOKENS, BLK), TOKENS ** -0.5, 0.25, ((0, 4), (1, 8)), (1, 2, 8, 2.0))
    return dict(owner_table=owner_table, hidden_acts=hidden_acts, sent_grad=sent_grad)


def inverse_root(gram):
    unit_matrix = jnp.eye(BLK, dtype=jnp.float32)
    shifted = gram + 1e-06 * unit_matrix
    norm_value = jnp.sqrt(jnp.sum(shifted * shifted))
    scaled = shifted / norm_value
    result = None
    for step_index in range(ITERS):
        factor = ((5.0 * unit_matrix - scaled) / 4.0).astype(jnp.bfloat16)
        if step_index == 0:
            result = factor
        else:
            result = jnp.dot(result, factor, preferred_element_type=jnp.float32).astype(jnp.bfloat16)
        if step_index + 1 < ITERS:
            square = jnp.dot(factor, factor, preferred_element_type=jnp.float32).astype(jnp.bfloat16)
            fourth = jnp.dot(square, square, preferred_element_type=jnp.float32).astype(jnp.bfloat16)
            scaled = jnp.dot(fourth, scaled.astype(jnp.bfloat16), preferred_element_type=jnp.float32)
    return result

def one_block(owned_block):
    left_gram = lax.dot_general(owned_block, owned_block, (((1,), (1,)), ((), ())), preferred_element_type=jnp.float32)
    right_gram = lax.dot_general(owned_block, owned_block, (((0,), (0,)), ((), ())), preferred_element_type=jnp.float32)
    left_root = inverse_root(left_gram)
    right_root = inverse_root(right_gram)
    projected = jnp.dot(left_root, owned_block, preferred_element_type=jnp.float32).astype(jnp.bfloat16)
    return jnp.dot(projected, right_root, preferred_element_type=jnp.float32).astype(jnp.bfloat16)

def one_section(packed):
    section_table, section_acts, section_grad = packed
    gradient = lax.dot_general(section_acts, section_grad, (((0,), (0,)), ((), ())), preferred_element_type=jnp.float32)
    blocks = gradient.reshape(NB, BLK, BLK).astype(jnp.bfloat16)
    owned_blocks = jnp.take(blocks, section_table.astype(jnp.int32), axis=0)
    return lax.map(one_block, owned_blocks)

def reference(owner_table, hidden_acts, sent_grad):
    incoming = jnp.roll(sent_grad, -1, axis=0)
    return lax.map(one_section, (owner_table, hidden_acts, incoming))
```

```python
import functools

import jax
import jax.numpy as jnp
from jax import lax
from jax.experimental import pallas as pl
from jax.experimental.pallas import tpu as pltpu
from jax.sharding import PartitionSpec as P

BLK = 512
ITERS = 2


def shifted_2(value, axis, steps):
    count = lax.axis_size(axis)
    pairs = [(source, (source + steps) % count) for source in range(count)]
    return lax.ppermute(value, axis, pairs)


def partner_2(block, axis, stride):
    count = lax.axis_size(axis)
    route = []
    for low in range(count):
        high = low | 1 << stride
        if high != low and high < count:
            route += [(low, high), (high, low)]
    return lax.ppermute(block, axis, route)


def inverse_root(gram):
    unit_matrix = jnp.eye(BLK, dtype=jnp.float32)
    shifted = gram + 1e-06 * unit_matrix
    norm_value = jnp.sqrt(jnp.sum(shifted * shifted))
    scaled = shifted / norm_value
    result = None
    for step_index in range(ITERS):
        factor = ((5.0 * unit_matrix - scaled) / 4.0).astype(jnp.bfloat16)
        if step_index == 0:
            result = factor
        else:
            result = jnp.dot(result, factor, preferred_element_type=jnp.float32).astype(
                jnp.bfloat16
            )
        if step_index + 1 < ITERS:
            square = jnp.dot(factor, factor, preferred_element_type=jnp.float32).astype(
                jnp.bfloat16
            )
            fourth = jnp.dot(square, square, preferred_element_type=jnp.float32).astype(
                jnp.bfloat16
            )
            scaled = jnp.dot(
                fourth, scaled.astype(jnp.bfloat16), preferred_element_type=jnp.float32
            )
    return result


def gram_rows(matrix):
    return lax.dot_general(
        matrix, matrix, (((1,), (1,)), ((), ())), preferred_element_type=jnp.float32
    )


def shards(owner_table, hidden_acts, sent_grad):
    owners_row = owner_table[0]
    block_count = owners_row.shape[0]
    replica_count = lax.axis_size("dp")
    group_size = replica_count // block_count
    row_count = BLK // group_size
    bit_count = group_size.bit_length() - 1
    my_index = lax.axis_index("dp")
    incoming = shifted_2(sent_grad[0], "section", -1)
    activations = hidden_acts[0]
    tokens = activations.shape[0]
    picked = jnp.take(activations.reshape(tokens, block_count, BLK), owners_row, axis=1)
    member = my_index % group_size
    offset = 0
    ordered = picked.reshape(tokens, block_count * BLK)
    summed = lax.psum_scatter(
        lax.dot_general(
            ordered, incoming, (((0,), (0,)), ((), ())), preferred_element_type=jnp.float32
        ),
        "dp",
        scatter_dimension=0,
        tiled=True,
    )
    owned_block = summed.astype(jnp.bfloat16)
    for bit_level in range(bit_count):
        partner = partner_2(owned_block, "dp", offset + bit_level)
        is_upper = member >> bit_level & 1 == 1
        owned_block = jnp.where(
            is_upper,
            jnp.concatenate([partner, owned_block], axis=0),
            jnp.concatenate([owned_block, partner], axis=0),
        )
    takes_right = member & 1 == 1
    operand = jnp.where(takes_right, owned_block.T, owned_block)
    own_root = inverse_root(gram_rows(operand))
    partner_root = partner_2(own_root, "dp", offset)
    left_root = jnp.where(takes_right, partner_root, own_root)
    right_root = jnp.where(takes_right, own_root, partner_root)
    left_rows = lax.dynamic_slice_in_dim(left_root, member * row_count, row_count, 0)
    projected = jnp.dot(left_rows, owned_block, preferred_element_type=jnp.float32).astype(
        jnp.bfloat16
    )
    my_update = jnp.dot(projected, right_root, preferred_element_type=jnp.float32).astype(
        jnp.bfloat16
    )
    gathered = lax.all_gather(my_update, "dp", axis=0, tiled=True)
    result_blocks = gathered.reshape(block_count, BLK, BLK)
    return result_blocks[None]

def line_routes(count, size):
    def devices(pairs):
        return [(a * size + m, b * size + m) for a, b in pairs for m in range(size)]

    half = count // 2
    routes = []
    for gap in range(1, count):
        up = [(low, low + gap) for low in range(count - gap)]
        down = [(high, low) for low, high in up]
        if gap < half:
            routes.append((gap, "direct", devices(up), devices(down)))
        elif gap == half:
            routes.append((gap, "half", devices(up + down), None))
        else:
            near = [(low + half, low + gap) for low in range(count - gap)]
            far = [(low + gap - half, low) for low in range(count - gap)]
            routes.append((gap, "relay", devices(near + far), None))
    return routes


def line_gather(value, axis, count, size):
    below, above = {}, {}
    middle = None
    for gap, kind, first, second in line_routes(count, size):
        if kind == "direct":
            below[gap] = lax.ppermute(value, axis, first)
            above[gap] = lax.ppermute(value, axis, second)
        elif kind == "half":
            middle = lax.ppermute(value, axis, first)
            below[gap] = above[gap] = middle
        else:
            below[gap] = above[gap] = lax.ppermute(middle, axis, first)
    return below, above


def matmul(left, right, dims=((1,), (0,))):
    return lax.dot_general(left, right, (dims, ((), ())), preferred_element_type=jnp.float32)


def pick_kernel(table, acts, out, sems):
    count, _, width = out.shape
    copies = []
    for slot in range(count):
        start = pl.multiple_of(table[slot] * width, width)
        copies.append(
            pltpu.make_async_copy(acts.at[:, pl.ds(start, width)], out.at[slot], sems.at[slot])
        )
    for copy in copies:
        copy.start()
    for copy in copies:
        copy.wait()


def partial_kernel(count, place, *refs):
    acts = refs[:count]
    grads = refs[count : 2 * count + count - 1]
    out = refs[-1]
    where = place[0]
    rows = [grads[0][...]]
    for turn in range(1, count):
        below, above = grads[2 * turn - 1][...], grads[2 * turn][...]
        rows.append(jnp.where(where >= turn, below, above))
    left = jnp.concatenate([ref[...] for ref in acts], axis=0)
    right = jnp.concatenate(rows, axis=0)
    out[...] = matmul(left, right, ((0,), (0,)))


def newton_root(gram):
    side = gram.shape[0]
    unit = (
        lax.broadcasted_iota(jnp.int32, (side, side), 0)
        == lax.broadcasted_iota(jnp.int32, (side, side), 1)
    ).astype(jnp.float32)
    shifted = gram + 1e-06 * unit
    scaled = shifted * (1.0 / jnp.sqrt(jnp.sum(shifted * shifted)))
    result = None
    for step_index in range(ITERS):
        factor = ((5.0 * unit - scaled) / 4.0).astype(jnp.bfloat16)
        if step_index == 0:
            result = factor
        else:
            result = matmul(result, factor).astype(jnp.bfloat16)
        if step_index + 1 < ITERS:
            square = matmul(factor, factor).astype(jnp.bfloat16)
            fourth = matmul(square, square).astype(jnp.bfloat16)
            scaled = matmul(fourth, scaled.astype(jnp.bfloat16))
    return result


def update_kernel(place, mine, other, out, left):
    owned = (mine[...] + other[...]).astype(jnp.bfloat16)
    flipped = owned.T
    left[...] = newton_root(matmul(owned, owned, ((1,), (1,))))
    right = newton_root(matmul(flipped, flipped, ((1,), (1,))))
    rows = out.shape[0]
    part = left[pl.ds(pl.multiple_of(place[1] * rows, rows), rows), :]
    projected = matmul(part, owned).astype(jnp.bfloat16)
    out[...] = matmul(projected, right).astype(jnp.bfloat16)


def place_kernel(count, place, *refs):
    pieces, out = refs[:-1], refs[-1]
    where, member = place[0], place[1]
    rows = pieces[0].shape[0]
    per_side = 1 + 2 * (count - 1)
    for side in range(2):
        side_pieces = pieces[side * per_side : (side + 1) * per_side]
        at = pl.multiple_of(jnp.where(member == side, 0, rows), rows)
        out[where, pl.ds(at, rows), :] = side_pieces[0][...]
        for gap in range(1, count):

            @pl.when(where >= gap)
            def _():
                out[where - gap, pl.ds(at, rows), :] = side_pieces[2 * gap - 1][...]

            @pl.when(where + gap < count)
            def _():
                out[where + gap, pl.ds(at, rows), :] = side_pieces[2 * gap][...]


def vmem_call(kernel, shape, dtype, operands, scratch=(), flops=0):
    vmem = pl.BlockSpec(memory_space=pltpu.VMEM)
    return pl.pallas_call(
        kernel,
        out_shape=jax.ShapeDtypeStruct(shape, dtype),
        in_specs=[pl.BlockSpec(memory_space=pltpu.SMEM)] + [vmem] * (len(operands) - 1),
        out_specs=vmem,
        scratch_shapes=list(scratch),
        cost_estimate=pl.CostEstimate(flops=flops, bytes_accessed=0, transcendentals=0),
    )(*operands)


def pair_shards(owner_table, hidden_acts, sent_grad):
    owners_row = owner_table[0]
    activations = hidden_acts[0]
    count = owners_row.shape[0]
    size = lax.axis_size("dp") // count
    tokens, width = activations.shape[0], sent_grad.shape[2]
    index = lax.axis_index("dp")
    where, member = index // size, index % size
    place = jnp.stack([where, member]).astype(jnp.int32)
    swap = [(low * size + m, low * size + (m ^ 1)) for low in range(count) for m in range(size)]

    incoming = shifted_2(sent_grad[0], "section", -1)
    turned = jnp.take(owners_row, (where + jnp.arange(count)) % count)
    picked = pl.pallas_call(
        pick_kernel,
        out_shape=jax.ShapeDtypeStruct((count, tokens, BLK), activations.dtype),
        in_specs=[pl.BlockSpec(memory_space=pltpu.SMEM), pl.BlockSpec(memory_space=pl.ANY)],
        out_specs=pl.BlockSpec(memory_space=pltpu.VMEM),
        scratch_shapes=[pltpu.SemaphoreType.DMA((count,))],
    )(turned, activations)
    acts = [picked[0]]
    for turn in range(1, count):
        route = [
            (low * size + m, (low + turn) % count * size + m)
            for low in range(count)
            for m in range(size)
        ]
        acts.append(lax.ppermute(picked[turn], "dp", route))
    below, above = line_gather(incoming, "dp", count, size)
    grads = [incoming]
    for turn in range(1, count):
        grads += [below[turn], above[count - turn]]
    part = vmem_call(
        functools.partial(partial_kernel, count),
        (BLK, width),
        jnp.float32,
        [place] + acts + grads,
        flops=2 * count * tokens * BLK * width,
    )
    other = lax.ppermute(part, "dp", swap)
    mine = vmem_call(
        update_kernel,
        (BLK // size, width),
        jnp.bfloat16,
        [place, part, other],
        scratch=[pltpu.VMEM((BLK, BLK), jnp.bfloat16)],
        flops=24 * BLK * BLK * width,
    )
    below, above = line_gather(mine, "dp", count, size)
    pieces = [mine]
    for gap in range(1, count):
        pieces += [below[gap], above[gap]]
    swapped = {id(piece): lax.ppermute(piece, "dp", swap) for piece in pieces}
    pieces += [swapped[id(piece)] for piece in pieces]
    result = vmem_call(
        functools.partial(place_kernel, count),
        (count, BLK, width),
        jnp.bfloat16,
        [place] + pieces,
    )
    return result[None]


def body(owner_table, hidden_acts, sent_grad):
    pairs = lax.axis_size("dp") == 2 * owner_table.shape[1]
    return (pair_shards if pairs else shards)(owner_table, hidden_acts, sent_grad)


def solution(mesh):
    return jax.shard_map(
        body,
        mesh=mesh,
        in_specs=(P("section", None), P("section", "dp", None), P("section", "dp", None)),
        out_specs=P("section", None, None, None),
        check_vma=False,
    )
```

```python
import functools

import jax
import jax.numpy as jnp
from jax import lax
from jax.experimental import pallas as pl
from jax.experimental.pallas import tpu as pltpu
from jax.sharding import PartitionSpec as P

BLK = 512
ITERS = 2


def shifted_2(value, axis, steps):
    count = lax.axis_size(axis)
    pairs = [(source, (source + steps) % count) for source in range(count)]
    return lax.ppermute(value, axis, pairs)


def partner_2(block, axis, stride):
    count = lax.axis_size(axis)
    route = []
    for low in range(count):
        high = low | 1 << stride
        if high != low and high < count:
            route += [(low, high), (high, low)]
    return lax.ppermute(block, axis, route)


def inverse_root(gram):
    unit_matrix = jnp.eye(BLK, dtype=jnp.float32)
    shifted = gram + 1e-06 * unit_matrix
    norm_value = jnp.sqrt(jnp.sum(shifted * shifted))
    scaled = shifted / norm_value
    result = None
    for step_index in range(ITERS):
        factor = ((5.0 * unit_matrix - scaled) / 4.0).astype(jnp.bfloat16)
        if step_index == 0:
            result = factor
        else:
            result = jnp.dot(result, factor, preferred_element_type=jnp.float32).astype(
                jnp.bfloat16
            )
        if step_index + 1 < ITERS:
            square = jnp.dot(factor, factor, preferred_element_type=jnp.float32).astype(
                jnp.bfloat16
            )
            fourth = jnp.dot(square, square, preferred_element_type=jnp.float32).astype(
                jnp.bfloat16
            )
            scaled = jnp.dot(
                fourth, scaled.astype(jnp.bfloat16), preferred_element_type=jnp.float32
            )
    return result


def gram_rows(matrix):
    return lax.dot_general(
        matrix, matrix, (((1,), (1,)), ((), ())), preferred_element_type=jnp.float32
    )


def shards(owner_table, hidden_acts, sent_grad):
    owners_row = owner_table[0]
    block_count = owners_row.shape[0]
    replica_count = lax.axis_size("dp")
    group_size = replica_count // block_count
    row_count = BLK // group_size
    bit_count = group_size.bit_length() - 1
    my_index = lax.axis_index("dp")
    incoming = shifted_2(sent_grad[0], "section", -1)
    activations = hidden_acts[0]
    tokens = activations.shape[0]
    picked = jnp.take(activations.reshape(tokens, block_count, BLK), owners_row, axis=1)
    member = my_index % group_size
    offset = 0
    ordered = picked.reshape(tokens, block_count * BLK)
    summed = lax.psum_scatter(
        lax.dot_general(
            ordered, incoming, (((0,), (0,)), ((), ())), preferred_element_type=jnp.float32
        ),
        "dp",
        scatter_dimension=0,
        tiled=True,
    )
    owned_block = summed.astype(jnp.bfloat16)
    for bit_level in range(bit_count):
        partner = partner_2(owned_block, "dp", offset + bit_level)
        is_upper = member >> bit_level & 1 == 1
        owned_block = jnp.where(
            is_upper,
            jnp.concatenate([partner, owned_block], axis=0),
            jnp.concatenate([owned_block, partner], axis=0),
        )
    takes_right = member & 1 == 1
    operand = jnp.where(takes_right, owned_block.T, owned_block)
    own_root = inverse_root(gram_rows(operand))
    partner_root = partner_2(own_root, "dp", offset)
    left_root = jnp.where(takes_right, partner_root, own_root)
    right_root = jnp.where(takes_right, own_root, partner_root)
    left_rows = lax.dynamic_slice_in_dim(left_root, member * row_count, row_count, 0)
    projected = jnp.dot(left_rows, owned_block, preferred_element_type=jnp.float32).astype(
        jnp.bfloat16
    )
    my_update = jnp.dot(projected, right_root, preferred_element_type=jnp.float32).astype(
        jnp.bfloat16
    )
    gathered = lax.all_gather(my_update, "dp", axis=0, tiled=True)
    result_blocks = gathered.reshape(block_count, BLK, BLK)
    return result_blocks[None]


def matmul(left, right, dims=((1,), (0,))):
    return lax.dot_general(left, right, (dims, ((), ())), preferred_element_type=jnp.float32)


def spot():
    return lax.axis_index("dp") // 2, lax.rem(lax.axis_index("dp"), 2)


def line_route(count, origins, start, gap):
    up = [(low + start, low + gap) for low in origins]
    pairs = [(2 * a, 2 * b) for a, b in up]
    return pairs + [(2 * (count - 1 - a) + 1, 2 * (count - 1 - b) + 1) for a, b in up]


def line_hops(count):
    half = count // 2
    hops = [("far", range(count - half - 1), 0, half)]
    hops += [("near", range(count - half - 1, count - half), 0, half)]
    hops += [(f"by{gap}", range(count - gap), 0, gap) for gap in range(1, half)]
    hops += [(f"on{gap}", range(count - gap), half, gap) for gap in range(half + 1, count)]
    return [hop for hop in hops if len(hop[1])]


def pick_kernel(count, first, table, acts, *refs):
    where, core = spot()
    *outs, owners, sem = refs
    outs = outs[-count:]
    tokens = acts.shape[0]
    copy = pltpu.make_async_copy(table, owners, sem.at[0])
    copy.start()
    copy.wait()
    width = outs[0].shape[1]
    for gap, out in enumerate(outs):
        target = jnp.clip(jnp.where(core == 0, where + gap, where - gap), 0, count - 1)
        columns = pl.ds(pl.multiple_of(owners[0, target] * width, width), width)
        out[0 if first else tokens : tokens if first else 2 * tokens] = acts[:, columns]


def join_kernel(low, high, out):
    out[: low.shape[0]] = low[...]
    out[low.shape[0] :] = high[...]


def unit_of(side):
    rows = lax.broadcasted_iota(jnp.int32, (side, side), 0)
    return (rows == lax.broadcasted_iota(jnp.int32, (side, side), 1)).astype(jnp.float32)


def factor_of(scaled, unit):
    return ((5.0 * unit - scaled) / 4.0).astype(jnp.bfloat16)


def normalized(gram, unit):
    shifted = gram + 1e-06 * unit
    return shifted * (1.0 / jnp.sqrt(jnp.sum(shifted * shifted)))


def update_kernel(terms, *refs):
    *pieces, out_low, out_high = refs
    total = None
    for acts, grads in terms:
        right = functools.reduce(lambda a, b: a + b, [pieces[at][...] for at in grads])
        term = matmul(pieces[acts][...], right, ((0,), (0,)))
        total = term if total is None else total + term
    owned = total.astype(jnp.bfloat16)
    flipped = owned.T
    unit = unit_of(owned.shape[0])
    scaled = [normalized(matmul(owned, flipped), unit), normalized(matmul(flipped, owned), unit)]
    roots = None
    for step_index in range(ITERS):
        factors = [factor_of(term, unit) for term in scaled]
        if step_index == 0:
            roots = factors
        else:
            roots = [matmul(a, b).astype(jnp.bfloat16) for a, b in zip(roots, factors)]
        if step_index + 1 < ITERS:
            squares = [matmul(a, a).astype(jnp.bfloat16) for a in factors]
            fourths = [matmul(a, a).astype(jnp.bfloat16) for a in squares]
            scaled = [matmul(a, b.astype(jnp.bfloat16)) for a, b in zip(fourths, scaled)]
    projected = matmul(roots[0], owned).astype(jnp.bfloat16)
    update = matmul(projected, roots[1]).astype(jnp.bfloat16)
    rows = out_low.shape[0]
    out_low[...] = update[:rows]
    out_high[...] = update[rows:]


def place_kernel(count, jobs, *refs):
    *pieces, out, sems = refs
    where, core = spot()
    rows = pieces[0].shape[0]
    at = 0
    copies = []
    for origins, gap, part in jobs:
        for mirrored in (False, True) if gap else (False,):
            up = core == (1 if mirrored else 0)
            block = jnp.where(up, where - gap, where + gap)
            rank = jnp.where(up, block, count - 1 - block)
            live = jnp.logical_and(rank >= origins[0], rank <= origins[-1])
            target = out.at[jnp.clip(block, 0, count - 1), pl.ds(part * rows, rows)]
            copies.append((live, pltpu.make_async_copy(pieces[at], target, sems.at[at])))
            at += 1
    for live, copy in copies:
        pl.when(live)(copy.start)
    for live, copy in copies:
        pl.when(live)(copy.wait)


VMEM = pl.BlockSpec(memory_space=pltpu.VMEM)
IN_HBM = pl.BlockSpec(memory_space=pltpu.HBM)
PARAMS = pltpu.CompilerParams(vmem_limit_bytes=24 * 2**20)


def cost(flops, moved):
    return pl.CostEstimate(flops=flops, bytes_accessed=moved, transcendentals=0)


def pair_shards(owner_table, hidden_acts, sent_grad):
    activations, outgoing = hidden_acts[0], sent_grad[0]
    count = owner_table.shape[1]
    tokens, width = outgoing.shape
    sections, replicas = lax.axis_size("section"), lax.axis_size("dp")
    swap_route = [(a, a ^ 1) for a in range(replicas)]

    def swap(piece):
        return lax.ppermute(piece, "dp", swap_route)

    def along(piece, route):
        return lax.ppermute(piece, "dp", route)

    def relayed(piece, route):
        pairs = [
            ((s + 1) % sections * replicas + a, s * replicas + b)
            for s in range(sections)
            for a, b in route
        ]
        return lax.ppermute(piece, ("section", "dp"), pairs)

    acts_other = swap(activations)
    grads_other = swap(outgoing)
    picked = ()
    for first, part in ((True, activations), (False, acts_other)):
        picked = pl.pallas_call(
            functools.partial(pick_kernel, count, first),
            out_shape=[jax.ShapeDtypeStruct((2 * tokens, BLK), activations.dtype)] * count,
            in_specs=[IN_HBM, VMEM] + [VMEM] * len(picked),
            out_specs=[VMEM] * count,
            input_output_aliases={2 + at: at for at in range(len(picked))},
            scratch_shapes=[
                pltpu.SMEM(owner_table.shape, owner_table.dtype),
                pltpu.SemaphoreType.DMA((1,)),
            ],
            compiler_params=PARAMS,
            cost_estimate=cost(10**6, 4 * activations.size),
        )(owner_table, part, *picked)
    joined = pl.pallas_call(
        join_kernel,
        out_shape=jax.ShapeDtypeStruct((2 * tokens, width), outgoing.dtype),
        in_specs=[VMEM] * 2,
        out_specs=VMEM,
        compiler_params=PARAMS,
        cost_estimate=cost(10**6, 4 * outgoing.size),
    )(outgoing, grads_other)
    grads = {0: [relayed(joined, [(a, a) for a in range(replicas)])]}
    acts = {0: picked[0]}
    for gap in range(1, count):
        acts[gap] = along(picked[gap], line_route(count, range(count - gap), 0, gap))
    middle = None
    for name, origins, start, gap in line_hops(count):
        route = line_route(count, origins, start, gap)
        if start:
            piece = along(middle, route)
        else:
            piece = relayed(joined, route)
        middle = piece if name == "far" else middle
        grads.setdefault(gap, []).append(piece)
    pieces, terms = [acts[0], *grads[0]], [(0, (1,))]
    for gap in range(1, count):
        for mirrored in (False, True):
            group = [acts[gap], *grads[gap]]
            if mirrored:
                group = [swap(piece) for piece in group]
            first = len(pieces)
            terms.append((first, tuple(range(first + 1, first + len(group)))))
            pieces += group
    own = pl.pallas_call(
        functools.partial(update_kernel, tuple(terms)),
        out_shape=[jax.ShapeDtypeStruct((BLK // 2, width), jnp.bfloat16)] * 2,
        in_specs=[VMEM] * len(pieces),
        out_specs=[VMEM] * 2,
        compiler_params=PARAMS,
        cost_estimate=cost(27 * BLK * BLK * width, 2**20),
    )(*pieces)
    pieces, jobs = list(own), [(range(count), 0, 0), (range(count), 0, 1)]
    for part in range(2):
        middle = None
        for name, origins, start, gap in line_hops(count):
            route = line_route(count, origins, start, gap)
            came = along(middle if start else own[part], route)
            middle = came if name == "far" else middle
            pieces += [came, swap(came)]
            jobs.append((origins, gap, part))
    result = pl.pallas_call(
        functools.partial(place_kernel, count, tuple(jobs)),
        out_shape=jax.ShapeDtypeStruct((count, BLK, width), jnp.bfloat16),
        in_specs=[VMEM] * len(pieces),
        out_specs=IN_HBM,
        scratch_shapes=[pltpu.SemaphoreType.DMA((len(pieces),))],
        compiler_params=PARAMS,
        cost_estimate=cost(10**6, 2 * count * BLK * width),
    )(*pieces)
    return result[None]


def body(owner_table, hidden_acts, sent_grad):
    if lax.axis_size("dp") != 2 * owner_table.shape[1]:
        return shards(owner_table, hidden_acts, sent_grad)
    return pair_shards(owner_table, hidden_acts, sent_grad)


def solution(mesh):
    return jax.shard_map(
        body,
        mesh=mesh,
        in_specs=(P("section", None), P("section", "dp", None), P("section", "dp", None)),
        out_specs=P("section", None, None, None),
        check_vma=False,
    )
```
